32 devices in a mesh: shot: 2 (over x), gz: 16 (over z, y, core).
Axes of the slice: x: 2, y: 2, z: 4, core: 2. Of those that a mesh axis runs over, the one named last changes fastest.
Arguments:
- source_now: float32 [256, 128, 128], P(('shot', 'gz')), parts along dimension 0, may hold values from -6 to 6
- source_before: float32 [256, 128, 128], P(('shot', 'gz')), parts along dimension 0, may hold values from -6 to 6
- receiver_now: float32 [256, 128, 128], P(('shot', 'gz')), parts along dimension 0, may hold values from -6 to 6
- receiver_before: float32 [256, 128, 128], P(('shot', 'gz')), parts along dimension 0, may hold values from -6 to 6
- speed_term: float32 [128, 128, 128], P('gz'), may hold values from 0.03 to 0.18
- saved_faces: float32 [24, 8, 128, 128], P('shot', None, 'gz'), parts along dimension 0, may hold values from -6 to 6
- face_steps: int32 [12], replicated, may hold values from 0 to 11, each once
- traces: bfloat16 [24, 128, 128], P('shot'), parts along dimension 0, may hold values from -6 to 6
- lag_offsets: int32 [8], replicated, may hold values from -8 to 8, as said below
- snap_phase: int32 [2], replicated, may hold values from 0 to 5
Outputs:
- image_out: bfloat16 [16, 128, 128, 128], P('shot', None, 'gz'), parts along dimension 0
- source_final: float32 [256, 128, 128], P(('shot', 'gz')), parts along dimension 0
- receiver_final: float32 [256, 128, 128], P(('shot', 'gz')), parts along dimension 0
The draws below stay inside these ranges and needn't reach their ends.
There are 2 independent parts, one for each index of `shot`. The reference program is written for one: setup_inputs(seed, part) draws one part's arguments, and reference() takes and returns one part's arrays. A program takes and returns all parts, laid end to end along the dimension named above; an argument that names none is the same for every part. Nothing has to cross between parts.
Inputs may be any that keep to these rules, and one draw needn't show every extreme that they name: `face_steps`: each of the 12 saved slots belongs to exactly one step. `lag_offsets`: the 8 offsets are different, and both ends of the range occur.
All inputs are finite; a program needn't handle non-finite values.
Results may differ from the reference program's by a relative error of at most 0.001.
Values sent between devices are 32-bit elements; how exact they have to be, the bound alone decides.
A program may use at most 64 MiB of HBM per device.

```python
import math
import jax
import jax.numpy as jnp
from jax import lax

NY = 128
NX = 128
LAGS = 8
LMAX = 8
STEPS = 12
SNAP_EVERY = 6
SNAPS = 2
NZ = 128


def draw_lag_offsets(key, part):
    first_key = jax.random.fold_in(key, 11)
    second_key = jax.random.fold_in(key, 12)
    interior = jax.random.permutation(first_key, 2 * LMAX - 1)[:LAGS - 2].astype(jnp.int32) - (LMAX - 1)
    ends_fixed = jnp.array([-LMAX, LMAX], jnp.int32)
    combined = jnp.concatenate([ends_fixed, interior])
    shuffle = jax.random.permutation(second_key, LAGS)
    return combined[shuffle]


def steps_of(key, extent, split, low, largest):
    factor_of = 1.0
    for position, shards_of in split:
        steps = jax.random.uniform(jax.random.fold_in(jax.random.fold_in(key, 6), position), (shards_of,), jnp.float32, low / len(split), largest / len(split))
        factor_of = factor_of * jnp.repeat(jnp.exp(steps), extent[position] // shards_of).reshape((-1,) + (1,) * (len(extent) - 1 - position))
    return factor_of


def gaussian(own_key, dims, spread, reach, split=(), kind=jnp.bfloat16):
    values = jax.random.normal(own_key, dims, jnp.float32) * spread
    if len(split) > 0:
        values = steps_of(own_key, dims, split, -0.22, 0.18) * values
    return jnp.clip(values, min=-reach, max=reach).astype(kind)


def setup_inputs(seed: int = 0, part: int = 0) -> dict:
    arg_keys = jax.random.split(jax.random.key(seed), 11)
    own_keys = jax.random.split(jax.random.fold_in(arg_keys[10], part), 11)
    source_now = gaussian(own_keys[0], (NZ, NY, NX), 1.0, 6.0, ((0, 16),), jnp.float32)
    source_before = gaussian(own_keys[1], (NZ, NY, NX), 1.0, 6.0, ((0, 16),), jnp.float32)
    receiver_now = gaussian(own_keys[2], (NZ, NY, NX), 1.0, 6.0, ((0, 16),), jnp.float32)
    receiver_before = gaussian(own_keys[3], (NZ, NY, NX), 1.0, 6.0, ((0, 16),), jnp.float32)
    speed_term = jnp.clip(jnp.exp(math.log(0.18) - 1.7917595 * jax.random.uniform(arg_keys[4], (NZ, NY, NX), jnp.float32) ** steps_of(arg_keys[4], (NZ, NY, NX), ((0, 16),), -0.2, 0.2)), 0.03, 0.18)
    saved_faces = gaussian(own_keys[5], (STEPS, 8, NZ, NY), 1.0, 6.0, ((2, 16),), jnp.float32)
    face_steps = jax.random.permutation(arg_keys[6], STEPS).astype(jnp.int32)
    traces = gaussian(own_keys[7], (STEPS, NY, NX), 1.0, 6.0)
    lag_offsets = draw_lag_offsets(jax.random.fold_in(arg_keys[10], 71), part)
    snap_phase = jax.random.randint(arg_keys[9], (SNAPS,), 0, SNAP_EVERY).astype(jnp.int32)
    return {"source_now": source_now, "source_before": source_before, "receiver_now": receiver_now, "receiver_before": receiver_before, "speed_term": speed_term, "saved_faces": saved_faces, "face_steps": face_steps, "traces": traces, "lag_offsets": lag_offsets, "snap_phase": snap_phase}


stencil_weights = (-205.0 / 72.0, 8.0 / 5.0, -1.0 / 5.0, 8.0 / 315.0, -1.0 / 560.0)
damping = 0.25
smoothing = 16.0

def stencil(extended, layers):
    center = extended[:, 4:4 + layers]
    height = center.shape[2]
    breadth = center.shape[3]
    padded = jnp.pad(center, ((0, 0), (0, 0), (4, 4), (4, 4)))
    summed = 3.0 * stencil_weights[0] * center
    for offset in range(1, 5):
        weight = stencil_weights[offset]
        summed = summed + weight * (extended[:, 4 + offset:4 + offset + layers] + extended[:, 4 - offset:4 - offset + layers])
        summed = summed + weight * (padded[:, :, 4 + offset:4 + offset + height, 4:4 + breadth] + padded[:, :, 4 - offset:4 - offset + height, 4:4 + breadth])
        summed = summed + weight * (padded[:, :, 4:4 + height, 4 + offset:4 + offset + breadth] + padded[:, :, 4:4 + height, 4 - offset:4 - offset + breadth])
    return summed

def advance(extended, center, previous, speed_term, faces_now, trace_now, top_row, layers):
    updated = 2.0 * center - previous + speed_term * stencil(extended, layers)
    left_faces = jnp.moveaxis(faces_now[:4], 0, -1)
    right_faces = jnp.moveaxis(faces_now[4:], 0, -1)
    source = updated[0].at[:, :, :4].set(left_faces).at[:, :, -4:].set(right_faces)
    top_mask = lax.broadcasted_iota(jnp.int32, (layers, 1, 1), 0) == top_row
    receiver = updated[1] + jnp.where(top_mask, trace_now[None], 0.0)
    return jnp.stack([source, receiver])

def lag_images(snapshot, lag_offsets):
    source = snapshot[0]
    receiver = snapshot[1]
    margin = ((0, 0), (0, 0), (LMAX, LMAX))
    source_pad = jnp.pad(source, margin)
    receiver_pad = jnp.pad(receiver, margin)
    breadth = source.shape[2]
    images = []
    for lag_index in range(LAGS):
        lag_now = lag_offsets[lag_index]
        shifted_source = lax.dynamic_slice_in_dim(source_pad, LMAX - lag_now, breadth, 2)
        shifted_receiver = lax.dynamic_slice_in_dim(receiver_pad, LMAX + lag_now, breadth, 2)
        images.append(shifted_source * shifted_receiver)
    return (jnp.stack(images), source * source)

def finish(raw_image, illumination):
    layers = illumination.shape[0]
    columns = illumination.reshape(layers, -1)
    lower = jnp.full((layers,), -smoothing, illumination.dtype).at[0].set(0.0)
    upper = jnp.full((layers,), -smoothing, illumination.dtype).at[-1].set(0.0)
    middle = jnp.full((layers,), 1.0 + 2.0 * smoothing, illumination.dtype)
    smooth = lax.linalg.tridiagonal_solve(lower, middle, upper, columns).reshape(illumination.shape)
    return (raw_image / (smooth + damping)).astype(jnp.bfloat16)

def reference(source_now, source_before, receiver_now, receiver_before, speed_term, saved_faces, face_steps, traces, lag_offsets, snap_phase):
    current = jnp.stack([source_now, receiver_now])
    previous = jnp.stack([source_before, receiver_before])
    layers = source_now.shape[0]
    zero_rows = jnp.zeros((2, 4) + source_now.shape[1:], source_now.dtype)
    raw_parts = []
    light_parts = []
    for window in range(SNAPS):
        snapshot = jnp.zeros_like(current)
        for local_index in range(SNAP_EVERY):
            step_index = window * SNAP_EVERY + local_index
            extended = jnp.concatenate([zero_rows, current, zero_rows], axis=1)
            updated = advance(extended, current, previous, speed_term, saved_faces[face_steps[step_index]], traces[step_index].astype(jnp.float32), 0, layers)
            snapshot = jnp.where(local_index == snap_phase[window], updated, snapshot)
            previous = current
            current = updated
        raw_now, light_now = lag_images(snapshot, lag_offsets)
        raw_parts.append(raw_now)
        light_parts.append(light_now)
    raw_image = raw_parts[0]
    illumination = light_parts[0]
    for window in range(1, SNAPS):
        raw_image = raw_image + raw_parts[window]
        illumination = illumination + light_parts[window]
    return (finish(raw_image, illumination), current[0], current[1])
```

```python
import functools

import jax
import jax.numpy as jnp
import numpy as np
from jax import lax
from jax.experimental import pallas as pl
from jax.experimental.pallas import tpu as pltpu
from jax.sharding import PartitionSpec as P

SNAP_EVERY = 6
SNAPS = 2
STEPS = SNAPS * SNAP_EVERY
HALO = 4
ROWS = 8
CHUNK = 4

stencil_weights = (-205.0 / 72.0, 8.0 / 5.0, -1.0 / 5.0, 8.0 / 315.0, -1.0 / 560.0)
damping = 0.25
smoothing = 16.0
MESH = pl.DeviceIdType.MESH


def lateral_weights(breadth):
    apart = np.abs(np.arange(breadth)[:, None] - np.arange(breadth)[None, :])
    band = np.zeros((breadth, breadth), np.float64)
    band[apart == 0] = 3.0 * stencil_weights[0]
    for offset in range(1, 5):
        band[apart == offset] = stencil_weights[offset]
    band = jnp.asarray(band, jnp.float32)
    high = band.astype(jnp.bfloat16)
    low = (band - high.astype(jnp.float32)).astype(jnp.bfloat16)
    return jnp.concatenate([high, high], axis=0), low


def wave_kernel(
    count,
    group,
    strip,
    phase_ref,
    src_now,
    src_old,
    rec_now,
    rec_old,
    speed,
    faces,
    traces,
    weights_a,
    weights_b,
    strips_out,
    src_out,
    rec_out,
    field,
    factor,
    edges,
    snaps,
    load_send,
    load_recv,
    load_own,
    halo_send,
    halo_recv,
    strip_send,
    strip_recv,
    strip_own,
    back_send,
    back_recv,
    back_own,
):
    me = lax.axis_index("gz")
    outer = count // group
    a = me // group
    b = me % group
    thin = src_now.shape[0]
    layers = thin * group
    height = src_now.shape[1] // group
    breadth = src_now.shape[2]
    inner = pl.ds(ROWS, height)

    def landing(index, sender):
        planes = pl.ds(HALO + sender * thin, thin)
        flat = pl.ds(sender * thin, thin)
        if index == 0:
            return factor.at[flat]
        if index == 5:
            return edges.at[flat]
        return {
            1: field.at[1, 0, planes, inner],
            2: field.at[1, 1, planes, inner],
            3: field.at[0, 0, planes, inner],
            4: field.at[0, 1, planes, inner],
        }[index]

    inputs = (speed, rec_now, rec_old, src_now, src_old, faces)

    def rows_of(quarter):
        return pl.ds(pl.multiple_of(quarter * height, ROWS), height)

    def load_copy(index, shift, sender, target):
        return pltpu.make_async_remote_copy(
            src_ref=inputs[index].at[:, rows_of(target), :],
            dst_ref=landing(index, sender),
            send_sem=load_send.at[index, shift],
            recv_sem=load_recv.at[index, shift],
            device_id={"gz": a * group + target},
            device_id_type=MESH,
        )

    def own_copy(index):
        return pltpu.make_async_copy(
            inputs[index].at[:, rows_of(b), :], landing(index, b), load_own.at[index]
        )

    for index in range(6):
        for shift in range(1, group):
            load_copy(index, shift, b, (b + shift) % group).start()
        own_copy(index).start()

    def wait_load(index):
        own_copy(index).wait()
        for shift in range(1, group):
            load_copy(index, shift, (b + group - shift) % group, b).wait_recv()

    def clear(where, value):
        for kind in range(2):
            for slot in range(2):
                field[(kind, slot) + where] = jnp.zeros(value, jnp.float32)

    @pl.when(a == 0)
    def _():
        clear((slice(0, HALO), slice(ROWS, ROWS + height)), (HALO, height, breadth))

    @pl.when(a == outer - 1)
    def _():
        clear(
            (slice(HALO + layers, 2 * HALO + layers), slice(ROWS, ROWS + height)),
            (HALO, height, breadth),
        )

    @pl.when(b == 0)
    def _():
        clear((slice(HALO, HALO + layers), slice(0, ROWS)), (layers, ROWS, breadth))

    @pl.when(b == group - 1)
    def _():
        clear(
            (slice(HALO, HALO + layers), slice(ROWS + height, 2 * ROWS + height)),
            (layers, ROWS, breadth),
        )

    snaps[...] = jnp.zeros(snaps.shape, jnp.float32)

    body = pl.ds(HALO, layers)
    to_next = (a < outer - 1, a > 0, b < group - 1, b > 0)
    from_prior = (a > 0, a < outer - 1, b > 0, b < group - 1)
    partner = (me + group, me - group, me + 1, me - 1)

    def halo_copy(kind, way, slot):
        view = field.at[kind, slot]
        source, target = (
            (view.at[pl.ds(layers, HALO), inner], view.at[pl.ds(0, HALO), inner]),
            (view.at[pl.ds(HALO, HALO), inner], view.at[pl.ds(HALO + layers, HALO), inner]),
            (view.at[body, pl.ds(height, ROWS)], view.at[body, pl.ds(0, ROWS)]),
            (view.at[body, pl.ds(ROWS, ROWS)], view.at[body, pl.ds(ROWS + height, ROWS)]),
        )[way]
        return pltpu.make_async_remote_copy(
            src_ref=source,
            dst_ref=target,
            send_sem=halo_send.at[kind, way, slot],
            recv_sem=halo_recv.at[kind, way, slot],
            device_id={"gz": partner[way]},
            device_id_type=MESH,
        )

    def send_halo(kind, way, slot, also=None):
        allowed = to_next[way] if also is None else jnp.logical_and(to_next[way], also)

        @pl.when(allowed)
        def _():
            halo_copy(kind, way, slot).start()

    def wait_halo(kind, way, slot):
        @pl.when(from_prior[way])
        def _():
            halo_copy(kind, way, slot).wait_recv()

    def wait_sent(kind, way, slot):
        @pl.when(to_next[way])
        def _():
            halo_copy(kind, way, slot).wait_send()

    lane = lax.broadcasted_iota(jnp.int32, (1, 1, breadth), 2)
    outside = (lane < 4) | (lane >= breadth - 4)

    def advance(kind, window, local, step, now, later, chunk, top):
        base = chunk * CHUNK
        planes = pl.ds(HALO + base, CHUNK)
        center = field[kind, now, planes, inner, :]
        flat = center.reshape(CHUNK * height, breadth)
        high = flat.astype(jnp.bfloat16)
        low = (flat - high.astype(jnp.float32)).astype(jnp.bfloat16)
        lateral = jnp.dot(
            jnp.concatenate([high, low], axis=1),
            weights_a[...],
            preferred_element_type=jnp.float32,
        ) + jnp.dot(high, weights_b[...], preferred_element_type=jnp.float32)
        summed = lateral.reshape(CHUNK, height, breadth)
        for offset in range(1, 5):
            summed = summed + stencil_weights[offset] * (
                (
                    field[kind, now, pl.ds(HALO + base + offset, CHUNK), inner, :]
                    + field[kind, now, pl.ds(HALO + base - offset, CHUNK), inner, :]
                )
                + (
                    field[kind, now, planes, pl.ds(ROWS + offset, height), :]
                    + field[kind, now, planes, pl.ds(ROWS - offset, height), :]
                )
            )
        previous = field[kind, later, planes, inner, :]
        updated = 2.0 * center - previous + factor[pl.ds(base, CHUNK)] * summed
        if kind == 0:
            placed = edges[pl.ds(base, CHUNK)].reshape(CHUNK * height, breadth)
            placed = pltpu.roll(placed, lax.rem(breadth - 8 * step, breadth), 1)
            updated = jnp.where(outside, placed.reshape(CHUNK, height, breadth), updated)
        elif top:
            updated = jnp.concatenate([updated[:1] + traces[step][None], updated[1:]], axis=0)
        field[kind, later, planes, inner, :] = updated
        held = snaps[window, kind, pl.ds(base, CHUNK)]
        take = phase_ref[window] == local
        snaps[window, kind, pl.ds(base, CHUNK)] = jnp.where(take, updated, held)

    chunks = layers // CHUNK

    def whole_step(kind, window, local):
        step = window * SNAP_EVERY + local
        now = lax.rem(step, 2)
        later = 1 - now
        more = step < STEPS - 1
        run = functools.partial(advance, kind, window, local, step, now, later)
        for way in range(4):
            wait_halo(kind, way, now)
        run(0, True)
        send_halo(kind, 1, later, more)
        run(chunks - 1, False)
        send_halo(kind, 0, later, more)

        def middle(chunk, carried):
            run(chunk, False)
            return carried

        lax.fori_loop(1, chunks - 1, middle, 0)
        send_halo(kind, 2, later, more)
        send_halo(kind, 3, later, more)
        for way in range(4):
            wait_sent(kind, way, now)

    def strip_copy(window, index, sender):
        target = b * outer + index
        first = pl.multiple_of(index * strip // ROWS * ROWS, ROWS)
        return (
            snaps.at[window, :, :, pl.ds(first, ROWS), :],
            strips_out.at[window, :, pl.ds(sender * layers, layers)],
            target,
        )

    def strip_remote(window, index, sender):
        source, landed, target = strip_copy(window, index, sender)
        return pltpu.make_async_remote_copy(
            src_ref=source,
            dst_ref=landed,
            send_sem=strip_send.at[window, index],
            recv_sem=strip_recv.at[window, sender],
            device_id={"gz": target},
            device_id_type=MESH,
        )

    def strip_local(window, index):
        source, landed, _ = strip_copy(window, index, a)
        return pltpu.make_async_copy(source, landed, strip_own.at[window])

    def start_strips(window):
        for turn in range(outer):
            index = (turn + a) % outer
            target = b * outer + index

            @pl.when(target != me)
            def _():
                strip_remote(window, index, a).start()

            @pl.when(target == me)
            def _():
                strip_local(window, index).start()

    def finish_strips(window):
        for turn in range(outer):
            index = (turn + a) % outer
            target = b * outer + index

            @pl.when(target != me)
            def _():
                strip_remote(window, index, a).wait_send()

            @pl.when(target == me)
            def _():
                strip_local(window, index).wait()

        quarter = me // outer
        for sender in range(outer):

            @pl.when(sender * group + quarter != me)
            def _():
                strip_remote(window, 0, sender).wait_recv()

    for index in (0, 1):
        wait_load(index)
    for way in range(4):
        send_halo(1, way, 0)
    for index in (3,):
        wait_load(index)
    for way in range(4):
        send_halo(0, way, 0)
    for index in (2, 4, 5):
        wait_load(index)
    for index in range(6):
        for shift in range(1, group):
            load_copy(index, shift, b, (b + shift) % group).wait_send()

    for window in range(SNAPS):

        def both(local, carried):
            whole_step(1, window, local)
            whole_step(0, window, local)
            return carried

        lax.fori_loop(0, SNAP_EVERY, both, 0)
        start_strips(window)

    last = STEPS % 2
    outs = (src_out, rec_out)

    def back_parts(kind, sender, target):
        return (
            field.at[kind, last, pl.ds(HALO + target * thin, thin), inner],
            outs[kind].at[:, rows_of(sender), :],
        )

    def back_copy(kind, shift, sender, target):
        source, landed = back_parts(kind, sender, target)
        return pltpu.make_async_remote_copy(
            src_ref=source,
            dst_ref=landed,
            send_sem=back_send.at[kind, shift],
            recv_sem=back_recv.at[kind, shift],
            device_id={"gz": a * group + target},
            device_id_type=MESH,
        )

    def back_local(kind):
        source, landed = back_parts(kind, b, b)
        return pltpu.make_async_copy(source, landed, back_own.at[kind])

    for kind in range(2):
        back_local(kind).start()
        for shift in range(1, group):
            back_copy(kind, shift, b, (b + shift) % group).start()
    for kind in range(2):
        back_local(kind).wait()
        for shift in range(1, group):
            back_copy(kind, shift, b, (b + shift) % group).wait_send()
            back_copy(kind, shift, (b + group - shift) % group, b).wait_recv()
    for window in range(SNAPS):
        finish_strips(window)


def image_kernel(lag_ref, pivot_ref, strips, image, inverse):
    depth = strips.shape[2]
    breadth = strips.shape[4]
    lags = image.shape[0]
    unit = strips.shape[3:]

    def down(z, carried):
        first = strips[0, 0, z]
        second = strips[1, 0, z]
        value = (first * first + second * second + smoothing * carried) * pivot_ref[z]
        inverse[z] = value
        return value

    lax.fori_loop(0, depth, down, jnp.zeros(unit, jnp.float32), unroll=8)

    def up(turn, carried):
        z = depth - 1 - turn
        value = inverse[z] + (smoothing * pivot_ref[z]) * carried
        inverse[z] = 1.0 / (value + damping)
        return value

    lax.fori_loop(0, depth, up, jnp.zeros(unit, jnp.float32), unroll=8)

    lane = lax.broadcasted_iota(jnp.int32, unit, 1)
    some = 8
    for index in range(lags):
        lag = lag_ref[index]
        reach = jnp.abs(lag)
        inside = (lane >= reach) & (lane < breadth - reach)
        back = lax.rem(2 * breadth - 2 * lag, breadth)
        forth = lax.rem(breadth + lag, breadth)

        def layers(block, carried):
            for part in range(some):
                z = block * some + part
                raw = strips[0, 0, z] * pltpu.roll(strips[0, 1, z], back, 1)
                raw = raw + strips[1, 0, z] * pltpu.roll(strips[1, 1, z], back, 1)
                raw = jnp.where(inside, pltpu.roll(raw, forth, 1), 0.0)
                image[index, z] = (raw * inverse[z]).astype(jnp.bfloat16)
            return carried

        lax.fori_loop(0, depth // some, layers, 0)


def local(
    count,
    source_now,
    source_before,
    receiver_now,
    receiver_before,
    speed_term,
    saved_faces,
    face_steps,
    traces,
    lag_offsets,
    snap_phase,
):
    thin, wide, breadth = source_now.shape
    group = 4
    outer = count // group
    layers = thin * group
    depth = thin * count
    height = wide // group
    strip = wide // count
    me = lax.axis_index("gz")

    ordered = jnp.take(saved_faces, face_steps, axis=0)
    ordered = jnp.concatenate([ordered[:, 4:], ordered[:, :4]], axis=1)
    ordered = ordered.reshape(STEPS * 8, thin * wide).T.reshape(thin, wide, STEPS * 8)
    faces = jnp.pad(ordered, ((0, 0), (0, 0), (0, breadth - STEPS * 8)))
    faces = jnp.concatenate([faces[:, :, 4:], faces[:, :, :4]], axis=2)

    rows = lax.dynamic_slice_in_dim(traces, (me % group) * height, height, 1)
    top = jnp.where(me // group == 0, rows.astype(jnp.float32), 0.0)
    weights_a, weights_b = lateral_weights(breadth)

    any_space = pl.BlockSpec(memory_space=pl.ANY)
    vmem = pl.BlockSpec(memory_space=pltpu.VMEM)
    smem = pl.BlockSpec(memory_space=pltpu.SMEM)
    dma = pltpu.SemaphoreType.DMA
    flat = jax.ShapeDtypeStruct(source_now.shape, jnp.float32)
    strips, source_final, receiver_final = pl.pallas_call(
        functools.partial(wave_kernel, count, group, strip),
        out_shape=(
            jax.ShapeDtypeStruct((SNAPS, 2, depth, ROWS, breadth), jnp.float32),
            flat,
            flat,
        ),
        in_specs=[smem] + [any_space] * 6 + [vmem] * 3,
        out_specs=(any_space, any_space, any_space),
        scratch_shapes=[
            pltpu.VMEM((2, 2, layers + 2 * HALO, height + 2 * ROWS, breadth), jnp.float32),
            pltpu.VMEM((layers, height, breadth), jnp.float32),
            pltpu.VMEM((layers, height, breadth), jnp.float32),
            pltpu.VMEM((SNAPS, 2, layers, height, breadth), jnp.float32),
            dma((6, group)),
            dma((6, group)),
            dma((6,)),
            dma((2, 4, 2)),
            dma((2, 4, 2)),
            dma((SNAPS, outer)),
            dma((SNAPS, outer)),
            dma((SNAPS,)),
            dma((2, group)),
            dma((2, group)),
            dma((2,)),
        ],
        compiler_params=pltpu.CompilerParams(
            has_side_effects=True, vmem_limit_bytes=40 * 1024 * 1024
        ),
        name="waves",
    )(
        snap_phase,
        source_now,
        source_before,
        receiver_now,
        receiver_before,
        speed_term,
        faces,
        top,
        weights_a,
        weights_b,
    )

    if strip < ROWS:
        strips = lax.dynamic_slice_in_dim(strips, (me * strip) % ROWS, strip, 3)
    pivots = []
    pivot = 0.0
    for _ in range(depth):
        pivot = 1.0 / (1.0 + 2.0 * smoothing - smoothing * smoothing * pivot)
        pivots.append(pivot)
    image = pl.pallas_call(
        image_kernel,
        out_shape=jax.ShapeDtypeStruct(
            (lag_offsets.shape[0], depth, strip, breadth), jnp.bfloat16
        ),
        in_specs=[smem, smem, vmem],
        out_specs=vmem,
        scratch_shapes=[pltpu.VMEM((depth, strip, breadth), jnp.float32)],
        compiler_params=pltpu.CompilerParams(vmem_limit_bytes=48 * 1024 * 1024),
        name="images",
    )(lag_offsets, jnp.asarray(np.array(pivots, np.float32)), strips)
    return image, source_final, receiver_final


def solution(mesh):
    return jax.shard_map(
        functools.partial(local, mesh.shape["gz"]),
        mesh=mesh,
        in_specs=(
            P(("shot", "gz"), None, None),
            P(("shot", "gz"), None, None),
            P(("shot", "gz"), None, None),
            P(("shot", "gz"), None, None),
            P("gz", None, None),
            P("shot", None, "gz", None),
            P(),
            P("shot", None, None),
            P(),
            P(),
        ),
        out_specs=(
            P("shot", None, "gz", None),
            P(("shot", "gz"), None, None),
            P(("shot", "gz"), None, None),
        ),
        check_vma=False,
    )
```

```python
import functools

import jax
import jax.numpy as jnp
import numpy as np
from jax import lax
from jax.experimental import pallas as pl
from jax.experimental.pallas import tpu as pltpu
from jax.sharding import PartitionSpec as P

SNAP_EVERY = 6
SNAPS = 2
STEPS = SNAPS * SNAP_EVERY
HALO = 4
ROWS = 8
CHUNK = 4

stencil_weights = (-205.0 / 72.0, 8.0 / 5.0, -1.0 / 5.0, 8.0 / 315.0, -1.0 / 560.0)
damping = 0.25
smoothing = 16.0
MESH = pl.DeviceIdType.MESH


def lateral_weights(breadth):
    apart = np.abs(np.arange(breadth)[:, None] - np.arange(breadth)[None, :])
    band = np.zeros((breadth, breadth), np.float64)
    band[apart == 0] = 3.0 * stencil_weights[0]
    for offset in range(1, 5):
        band[apart == offset] = stencil_weights[offset]
    band = jnp.asarray(band, jnp.float32)
    high = band.astype(jnp.bfloat16)
    low = (band - high.astype(jnp.float32)).astype(jnp.bfloat16)
    return jnp.concatenate([high, high], axis=0), low


def wave_kernel(
    count,
    group,
    strip,
    phase_ref,
    src_now,
    src_old,
    rec_now,
    rec_old,
    speed,
    faces,
    traces,
    weights_a,
    weights_b,
    strips_out,
    src_out,
    rec_out,
    field,
    factor,
    edges,
    snaps,
    load_send,
    load_recv,
    load_own,
    halo_send,
    halo_recv,
    strip_send,
    strip_recv,
    strip_own,
    back_send,
    back_recv,
    back_own,
):
    me = lax.axis_index("gz")
    outer = count // group
    a = me // group
    b = me % group
    q = (group - b) % group
    thin = src_now.shape[0]
    layers = thin * group
    height = src_now.shape[1] // group
    breadth = src_now.shape[2]
    inner = pl.ds(ROWS, height)

    def landing(index, sender):
        planes = pl.ds(HALO + sender * thin, thin)
        flat = pl.ds(sender * thin, thin)
        if index == 0:
            return factor.at[flat]
        if index == 5:
            return edges.at[flat]
        return {
            1: field.at[1, 0, planes, inner],
            2: field.at[1, 1, planes, inner],
            3: field.at[0, 0, planes, inner],
            4: field.at[0, 1, planes, inner],
        }[index]

    inputs = (speed, rec_now, rec_old, src_now, src_old, faces)

    def rows_of(quarter):
        return pl.ds(pl.multiple_of(quarter * height, ROWS), height)

    def load_copy(index, shift, sender, target):
        return pltpu.make_async_remote_copy(
            src_ref=inputs[index].at[:, rows_of((group - target) % group), :],
            dst_ref=landing(index, sender),
            send_sem=load_send.at[index, shift],
            recv_sem=load_recv.at[index, shift],
            device_id={"gz": a * group + target},
            device_id_type=MESH,
        )

    def own_copy(index):
        return pltpu.make_async_copy(
            inputs[index].at[:, rows_of(q), :], landing(index, b), load_own.at[index]
        )

    for index in range(6):
        for shift in range(1, group):
            load_copy(index, shift, b, (b + shift) % group).start()
        own_copy(index).start()

    def wait_load(index):
        own_copy(index).wait()
        for shift in range(1, group):
            load_copy(index, shift, (b + group - shift) % group, b).wait_recv()

    def clear(where, value):
        for kind in range(2):
            for slot in range(2):
                field[(kind, slot) + where] = jnp.zeros(value, jnp.float32)

    @pl.when(a == 0)
    def _():
        clear((slice(0, HALO), slice(ROWS, ROWS + height)), (HALO, height, breadth))

    @pl.when(a == outer - 1)
    def _():
        clear(
            (slice(HALO + layers, 2 * HALO + layers), slice(ROWS, ROWS + height)),
            (HALO, height, breadth),
        )

    @pl.when(q == 0)
    def _():
        clear((slice(HALO, HALO + layers), slice(0, ROWS)), (layers, ROWS, breadth))

    @pl.when(q == group - 1)
    def _():
        clear(
            (slice(HALO, HALO + layers), slice(ROWS + height, 2 * ROWS + height)),
            (layers, ROWS, breadth),
        )

    snaps[...] = jnp.zeros(snaps.shape, jnp.float32)

    body = pl.ds(HALO, layers)
    to_next = (a < outer - 1, a > 0, q < group - 1, q > 0)
    from_prior = (a > 0, a < outer - 1, q > 0, q < group - 1)
    partner = (
        me + group,
        me - group,
        a * group + (2 * group - q - 1) % group,
        a * group + (group - q + 1) % group,
    )

    def halo_copy(kind, way, slot):
        view = field.at[kind, slot]
        source, target = (
            (view.at[pl.ds(layers, HALO), inner], view.at[pl.ds(0, HALO), inner]),
            (view.at[pl.ds(HALO, HALO), inner], view.at[pl.ds(HALO + layers, HALO), inner]),
            (view.at[body, pl.ds(ROWS + height - HALO, HALO)], view.at[body, pl.ds(ROWS - HALO, HALO)]),
            (view.at[body, pl.ds(ROWS, HALO)], view.at[body, pl.ds(ROWS + height, HALO)]),
        )[way]
        return pltpu.make_async_remote_copy(
            src_ref=source,
            dst_ref=target,
            send_sem=halo_send.at[kind, way, slot],
            recv_sem=halo_recv.at[kind, way, slot],
            device_id={"gz": partner[way]},
            device_id_type=MESH,
        )

    def send_halo(kind, way, slot, also=None):
        allowed = to_next[way] if also is None else jnp.logical_and(to_next[way], also)

        @pl.when(allowed)
        def _():
            halo_copy(kind, way, slot).start()

    def wait_halo(kind, way, slot):
        @pl.when(from_prior[way])
        def _():
            halo_copy(kind, way, slot).wait_recv()

    def wait_sent(kind, way, slot):
        @pl.when(to_next[way])
        def _():
            halo_copy(kind, way, slot).wait_send()

    lane = lax.broadcasted_iota(jnp.int32, (1, 1, breadth), 2)
    outside = (lane < 4) | (lane >= breadth - 4)

    def advance(kind, window, local, step, now, later, chunk, top):
        base = chunk * CHUNK
        planes = pl.ds(HALO + base, CHUNK)
        center = field[kind, now, planes, inner, :]
        flat = center.reshape(CHUNK * height, breadth)
        high = flat.astype(jnp.bfloat16)
        low = (flat - high.astype(jnp.float32)).astype(jnp.bfloat16)
        lateral = jnp.dot(
            jnp.concatenate([high, low], axis=1),
            weights_a[...],
            preferred_element_type=jnp.float32,
        ) + jnp.dot(high, weights_b[...], preferred_element_type=jnp.float32)
        summed = lateral.reshape(CHUNK, height, breadth)
        for offset in range(1, 5):
            summed = summed + stencil_weights[offset] * (
                (
                    field[kind, now, pl.ds(HALO + base + offset, CHUNK), inner, :]
                    + field[kind, now, pl.ds(HALO + base - offset, CHUNK), inner, :]
                )
                + (
                    field[kind, now, planes, pl.ds(ROWS + offset, height), :]
                    + field[kind, now, planes, pl.ds(ROWS - offset, height), :]
                )
            )
        previous = field[kind, later, planes, inner, :]
        updated = 2.0 * center - previous + factor[pl.ds(base, CHUNK)] * summed
        if kind == 0:
            placed = edges[pl.ds(base, CHUNK)].reshape(CHUNK * height, breadth)
            placed = pltpu.roll(placed, lax.rem(breadth - 8 * step, breadth), 1)
            updated = jnp.where(outside, placed.reshape(CHUNK, height, breadth), updated)
        elif top:
            updated = jnp.concatenate([updated[:1] + traces[step][None], updated[1:]], axis=0)
        field[kind, later, planes, inner, :] = updated
        held = snaps[window, kind, pl.ds(base, CHUNK)]
        take = phase_ref[window] == local
        snaps[window, kind, pl.ds(base, CHUNK)] = jnp.where(take, updated, held)

    chunks = layers // CHUNK

    def whole_step(kind, window, local):
        step = window * SNAP_EVERY + local
        now = lax.rem(step, 2)
        later = 1 - now
        more = step < STEPS - 1
        run = functools.partial(advance, kind, window, local, step, now, later)
        for way in range(4):
            wait_halo(kind, way, now)
        run(0, True)
        send_halo(kind, 1, later, more)
        run(chunks - 1, False)
        send_halo(kind, 0, later, more)

        def middle(chunk, carried):
            run(chunk, False)
            return carried

        lax.fori_loop(1, chunks - 1, middle, 0)
        send_halo(kind, 2, later, more)
        send_halo(kind, 3, later, more)
        for way in range(4):
            wait_sent(kind, way, now)

    def strip_copy(window, index, sender):
        target = q * outer + index
        first = pl.multiple_of(index * strip // ROWS * ROWS, ROWS)
        return (
            snaps.at[window, :, :, pl.ds(first, ROWS), :],
            strips_out.at[window, :, pl.ds(sender * layers, layers)],
            target,
        )

    def strip_remote(window, index, sender):
        source, landed, target = strip_copy(window, index, sender)
        return pltpu.make_async_remote_copy(
            src_ref=source,
            dst_ref=landed,
            send_sem=strip_send.at[window, index],
            recv_sem=strip_recv.at[window, sender],
            device_id={"gz": target},
            device_id_type=MESH,
        )

    def strip_local(window, index):
        source, landed, _ = strip_copy(window, index, a)
        return pltpu.make_async_copy(source, landed, strip_own.at[window])

    def start_strip(window, turn):
        index = (turn + a) % outer
        target = q * outer + index

        @pl.when(jnp.logical_and(target != me, turn < outer))
        def _():
            strip_remote(window, index, a).start()

        @pl.when(jnp.logical_and(target == me, turn < outer))
        def _():
            strip_local(window, index).start()

    def finish_strips(window):
        for turn in range(outer):
            index = (turn + a) % outer
            target = q * outer + index

            @pl.when(target != me)
            def _():
                strip_remote(window, index, a).wait_send()

            @pl.when(target == me)
            def _():
                strip_local(window, index).wait()

        quarter = me // outer
        for sender in range(outer):

            @pl.when(sender * group + (group - quarter) % group != me)
            def _():
                strip_remote(window, 0, sender).wait_recv()

    for index in (0, 1):
        wait_load(index)
    for way in range(4):
        send_halo(1, way, 0)
    for index in (3,):
        wait_load(index)
    for way in range(4):
        send_halo(0, way, 0)
    for index in (2, 4, 5):
        wait_load(index)
    for index in range(6):
        for shift in range(1, group):
            load_copy(index, shift, b, (b + shift) % group).wait_send()

    share = (outer + SNAP_EVERY - 1) // SNAP_EVERY
    for window in range(SNAPS):

        def both(local, carried):
            whole_step(1, window, local)
            whole_step(0, window, local)
            if window > 0:
                for part in range(share):
                    start_strip(window - 1, local * share + part)
            return carried

        lax.fori_loop(0, SNAP_EVERY, both, 0)
    for turn in range(outer):
        start_strip(SNAPS - 1, turn)

    last = STEPS % 2
    outs = (src_out, rec_out)

    def back_parts(kind, sender, target):
        return (
            field.at[kind, last, pl.ds(HALO + target * thin, thin), inner],
            outs[kind].at[:, rows_of((group - sender) % group), :],
        )

    def back_copy(kind, shift, sender, target):
        source, landed = back_parts(kind, sender, target)
        return pltpu.make_async_remote_copy(
            src_ref=source,
            dst_ref=landed,
            send_sem=back_send.at[kind, shift],
            recv_sem=back_recv.at[kind, shift],
            device_id={"gz": a * group + target},
            device_id_type=MESH,
        )

    def back_local(kind):
        source, landed = back_parts(kind, b, b)
        return pltpu.make_async_copy(source, landed, back_own.at[kind])

    for kind in range(2):
        back_local(kind).start()
        for shift in range(1, group):
            back_copy(kind, shift, b, (b + shift) % group).start()
    for kind in range(2):
        back_local(kind).wait()
        for shift in range(1, group):
            back_copy(kind, shift, b, (b + shift) % group).wait_send()
            back_copy(kind, shift, (b + group - shift) % group, b).wait_recv()
    for window in range(SNAPS):
        finish_strips(window)


def image_kernel(lag_ref, pivot_ref, strips, image, inverse):
    depth = strips.shape[2]
    breadth = strips.shape[4]
    lags = image.shape[0]
    unit = strips.shape[3:]

    def down(z, carried):
        first = strips[0, 0, z]
        second = strips[1, 0, z]
        value = (first * first + second * second + smoothing * carried) * pivot_ref[z]
        inverse[z] = value
        return value

    lax.fori_loop(0, depth, down, jnp.zeros(unit, jnp.float32), unroll=8)

    def up(turn, carried):
        z = depth - 1 - turn
        value = inverse[z] + (smoothing * pivot_ref[z]) * carried
        inverse[z] = 1.0 / (value + damping)
        return value

    lax.fori_loop(0, depth, up, jnp.zeros(unit, jnp.float32), unroll=8)

    lane = lax.broadcasted_iota(jnp.int32, unit, 1)
    some = 32
    for index in range(lags):
        lag = lag_ref[index]
        reach = jnp.abs(lag)
        inside = (lane >= reach) & (lane < breadth - reach)
        back = lax.rem(2 * breadth - 2 * lag, breadth)
        forth = lax.rem(breadth + lag, breadth)

        def layers(block, carried):
            z = pl.ds(block * some, some)
            raw = strips[0, 0, z] * pltpu.roll(strips[0, 1, z], back, 2)
            raw = raw + strips[1, 0, z] * pltpu.roll(strips[1, 1, z], back, 2)
            raw = jnp.where(inside[None], pltpu.roll(raw, forth, 2), 0.0)
            image[index, z] = (raw * inverse[z]).astype(jnp.bfloat16)
            return carried

        lax.fori_loop(0, depth // some, layers, 0)


def local(
    count,
    source_now,
    source_before,
    receiver_now,
    receiver_before,
    speed_term,
    saved_faces,
    face_steps,
    traces,
    lag_offsets,
    snap_phase,
):
    thin, wide, breadth = source_now.shape
    group = 4
    outer = count // group
    layers = thin * group
    depth = thin * count
    height = wide // group
    strip = wide // count
    me = lax.axis_index("gz")

    ordered = jnp.take(saved_faces, face_steps, axis=0)
    ordered = jnp.concatenate([ordered[:, 4:], ordered[:, :4]], axis=1)
    ordered = ordered.reshape(STEPS * 8, thin * wide).T.reshape(thin, wide, STEPS * 8)
    faces = jnp.pad(ordered, ((0, 0), (0, 0), (0, breadth - STEPS * 8)))
    faces = jnp.concatenate([faces[:, :, 4:], faces[:, :, :4]], axis=2)

    rows = lax.dynamic_slice_in_dim(traces, (group - me % group) % group * height, height, 1)
    top = jnp.where(me // group == 0, rows.astype(jnp.float32), 0.0)
    weights_a, weights_b = lateral_weights(breadth)

    any_space = pl.BlockSpec(memory_space=pl.ANY)
    vmem = pl.BlockSpec(memory_space=pltpu.VMEM)
    smem = pl.BlockSpec(memory_space=pltpu.SMEM)
    dma = pltpu.SemaphoreType.DMA
    flat = jax.ShapeDtypeStruct(source_now.shape, jnp.float32)
    strips, source_final, receiver_final = pl.pallas_call(
        functools.partial(wave_kernel, count, group, strip),
        out_shape=(
            jax.ShapeDtypeStruct((SNAPS, 2, depth, ROWS, breadth), jnp.float32),
            flat,
            flat,
        ),
        in_specs=[smem] + [any_space] * 6 + [vmem] * 3,
        out_specs=(any_space, any_space, any_space),
        scratch_shapes=[
            pltpu.VMEM((2, 2, layers + 2 * HALO, height + 2 * ROWS, breadth), jnp.float32),
            pltpu.VMEM((layers, height, breadth), jnp.float32),
            pltpu.VMEM((layers, height, breadth), jnp.float32),
            pltpu.VMEM((SNAPS, 2, layers, height, breadth), jnp.float32),
            dma((6, group)),
            dma((6, group)),
            dma((6,)),
            dma((2, 4, 2)),
            dma((2, 4, 2)),
            dma((SNAPS, outer)),
            dma((SNAPS, outer)),
            dma((SNAPS,)),
            dma((2, group)),
            dma((2, group)),
            dma((2,)),
        ],
        compiler_params=pltpu.CompilerParams(
            has_side_effects=True, vmem_limit_bytes=40 * 1024 * 1024
        ),
        name="waves",
    )(
        snap_phase,
        source_now,
        source_before,
        receiver_now,
        receiver_before,
        speed_term,
        faces,
        top,
        weights_a,
        weights_b,
    )

    if strip < ROWS:
        strips = lax.dynamic_slice_in_dim(strips, (me * strip) % ROWS, strip, 3)
    pivots = []
    pivot = 0.0
    for _ in range(depth):
        pivot = 1.0 / (1.0 + 2.0 * smoothing - smoothing * smoothing * pivot)
        pivots.append(pivot)
    image = pl.pallas_call(
        image_kernel,
        out_shape=jax.ShapeDtypeStruct(
            (lag_offsets.shape[0], depth, strip, breadth), jnp.bfloat16
        ),
        in_specs=[smem, smem, vmem],
        out_specs=vmem,
        scratch_shapes=[pltpu.VMEM((depth, strip, breadth), jnp.float32)],
        compiler_params=pltpu.CompilerParams(vmem_limit_bytes=48 * 1024 * 1024),
        name="images",
    )(lag_offsets, jnp.asarray(np.array(pivots, np.float32)), strips)
    return image, source_final, receiver_final


def solution(mesh):
    return jax.shard_map(
        functools.partial(local, mesh.shape["gz"]),
        mesh=mesh,
        in_specs=(
            P(("shot", "gz"), None, None),
            P(("shot", "gz"), None, None),
            P(("shot", "gz"), None, None),
            P(("shot", "gz"), None, None),
            P("gz", None, None),
            P("shot", None, "gz", None),
            P(),
            P("shot", None, None),
            P(),
            P(),
        ),
        out_specs=(
            P("shot", None, "gz", None),
            P(("shot", "gz"), None, None),
            P(("shot", "gz"), None, None),
        ),
        check_vma=False,
    )
```
